512 devices in a mesh: groups: 2 (over y), seq: 16 (over z), head: 8 (over x), rep: 2 (over core).
Axes of the slice: x: 8, y: 2, z: 16, core: 2. Of those that a mesh axis runs over, the one named last changes fastest.
The devices are a block of a 8x8x16 slice.
Arguments:
- queries: bfloat16 [512, 64, 128], P(('groups', 'seq', 'rep'), 'head'), parts along dimension 0, may hold values from -256 to 256
- page_owner: int32 [512, 128], P(('groups', 'seq', 'rep')), parts along dimension 0, may hold values from -1 to 15, as said below
- page_slot: int32 [512, 128], P(('groups', 'seq', 'rep')), parts along dimension 0, may hold values from -1 to 63, as said below
- lengths: int32 [512], P(('groups', 'seq', 'rep')), parts along dimension 0, may hold values from 1 to 16384, as said below
- keys: bfloat16 [4096, 8, 128, 128], P(('groups', 'seq', 'rep'), 'head'), parts along dimension 0, may hold values from -24 to 24
- values: bfloat16 [4096, 8, 128, 128], P(('groups', 'seq', 'rep'), 'head'), parts along dimension 0, may hold values from -6 to 6
Outputs:
- attended: bfloat16 [512, 64, 128], P(('groups', 'seq', 'rep'), 'head'), parts along dimension 0
The draws below stay inside these ranges and needn't reach their ends.
There are 2 independent parts, one for each index of `groups`. The reference program is written for one: setup_inputs(seed, part) draws one part's arguments, and reference() takes and returns one part's arrays. A program takes and returns all parts, laid end to end along the dimension named above; each array names one. Nothing has to cross between parts.
Inputs may be any that keep to these rules, and one draw needn't show every extreme that they name: `page_owner`: for j below ceil(lengths[r] / 128) the seq index of the device, among those of r's half (r // 8) % 2, whose pool holds page j of r; -1 for later j. `page_slot`: the page's slot in that pool, -1 where page_owner is -1. No slot of a pool holds two pages; in each half, some device's pool has all 64 slots in use. `lengths`: in each half some request has the most.
All inputs are finite; a program needn't handle non-finite values.
Results may differ from the reference program's by a relative error of at most 0.0041.
Values may be sent and summed in bfloat16 or wider, within the bound.
No kernel may reach another device: no remote copies, remote signals or barrier semaphores. Data moves between devices by JAX's collectives and lax.ppermute only.
A program may use at most 64 MiB of HBM per device.

```python
import math
import jax
import jax.numpy as jnp
from jax import lax

QH = 64
KVH = 8
HD = 128
PAGE = 128
MAXP = 128
REQ_DEV = 8
POOL_DEV = 64
REQ = 256
N_SEQ = 16
N_REP = 2


def page_layout(key):
    rows_half = REQ_DEV * N_SEQ
    total_pages = POOL_DEV * (N_SEQ + 1) // 2
    spare_pages = total_pages - rows_half
    extra_cells = rows_half * (MAXP - 1)
    slots_all = N_SEQ * POOL_DEV
    owner_list = []
    slot_list = []
    length_list = []
    for half_index in range(N_REP):
        half_keys = jax.random.split(jax.random.fold_in(key, 101 + half_index), 6)
        longest = jax.random.randint(half_keys[0], (), 0, rows_half)
        shuffled = jax.random.permutation(half_keys[1], extra_cells).astype(jnp.int32)
        cell_row = jnp.arange(extra_cells, dtype=jnp.int32) // (MAXP - 1)
        priority = jnp.where(cell_row == longest, shuffled - extra_cells, shuffled)
        ranked = jnp.argsort(priority)
        chosen = jnp.zeros((extra_cells,), jnp.int32).at[ranked[:spare_pages]].set(1)
        page_count = 1 + jnp.sum(chosen.reshape(rows_half, MAXP - 1), axis=1)
        tail_tokens = jax.random.randint(half_keys[2], (rows_half,), 1, PAGE + 1)
        tail_tokens = jnp.where(jnp.arange(rows_half) == longest, PAGE, tail_tokens)
        length_list.append((page_count - 1) * PAGE + tail_tokens)
        device_weight = jax.random.randint(half_keys[3], (N_SEQ,), 2, 5)
        lightest = jax.random.randint(half_keys[4], (), 0, N_SEQ)
        device_weight = jnp.where(jnp.arange(N_SEQ) == lightest, 1, device_weight)
        tie_break = jax.random.permutation(half_keys[5], slots_all).astype(jnp.int32)
        slot_ids = jnp.arange(slots_all, dtype=jnp.int32)
        slot_score = slot_ids % POOL_DEV * device_weight[slot_ids // POOL_DEV] * slots_all + tie_break
        picked = jnp.argsort(slot_score)[:total_pages].astype(jnp.int32)
        first_page = jnp.cumsum(page_count) - page_count
        page_index = jnp.arange(MAXP, dtype=jnp.int32)
        page_used = page_index[None, :] < page_count[:, None]
        flat_index = jnp.clip(first_page[:, None] + page_index[None, :], 0, total_pages - 1)
        chosen_slot = picked[flat_index]
        owner_list.append(jnp.where(page_used, chosen_slot // POOL_DEV, -1))
        slot_list.append(jnp.where(page_used, chosen_slot % POOL_DEV, -1))

    def arrange(pieces):
        tail_shape = pieces[0].shape[1:]
        stacked = jnp.stack(pieces).reshape((N_REP, N_SEQ, REQ_DEV) + tail_shape)
        stacked = jnp.moveaxis(stacked, 0, 1)
        return stacked.reshape((REQ,) + tail_shape).astype(jnp.int32)
    return (arrange(owner_list), arrange(slot_list), arrange(length_list))


def draw_page_owner(key, part):
    return page_layout(key)[0]


def draw_page_slot(key, part):
    return page_layout(key)[1]


def draw_lengths(key, part):
    return page_layout(key)[2]


def draw_keys(key, part):
    full_shape = (N_SEQ * N_REP * POOL_DEV, KVH, PAGE, HD)
    sample = jax.random.normal(jax.random.fold_in(key, 11), full_shape, jnp.float32)
    return jnp.clip(sample, -24.0, 24.0).astype(jnp.bfloat16)


def draw_queries(key, part):
    full_shape = (REQ, QH, HD)
    sample = jax.random.normal(jax.random.fold_in(key, 23), full_shape, jnp.float32)
    return jnp.clip(sample, -256.0, 256.0).astype(jnp.bfloat16)


def levels(rng, dims, cuts, least, top_value):
    gain = 1.0
    for dim, shards_of in cuts:
        heights = jax.random.uniform(jax.random.fold_in(jax.random.fold_in(rng, 6), dim), (shards_of,), jnp.float32, least / len(cuts), top_value / len(cuts))
        gain = gain * jnp.repeat(jnp.exp(heights), dims[dim] // shards_of).reshape((-1,) + (1,) * (len(dims) - 1 - dim))
    return gain


def bell_draw(stream_key, dims, scale, bound, cuts=(), kind=jnp.bfloat16):
    result = jax.random.normal(stream_key, dims, jnp.float32) * scale
    if len(cuts) > 0:
        result = levels(stream_key, dims, cuts, -0.22, 0.18) * result
    return jnp.clip(result, min=-bound, max=bound).astype(kind)


def setup_inputs(seed: int = 0, part: int = 0) -> dict:
    key_of = jax.random.split(jax.random.key(seed), 7)
    part_splits = jax.random.split(jax.random.fold_in(key_of[6], part), 7)
    queries = draw_queries(jax.random.fold_in(jax.random.fold_in(key_of[6], part), 71), part)
    page_owner = draw_page_owner(jax.random.fold_in(jax.random.fold_in(key_of[6], part), 71), part)
    page_slot = draw_page_slot(jax.random.fold_in(jax.random.fold_in(key_of[6], part), 71), part)
    lengths = draw_lengths(jax.random.fold_in(jax.random.fold_in(key_of[6], part), 71), part)
    keys = draw_keys(jax.random.fold_in(jax.random.fold_in(key_of[6], part), 71), part)
    values = bell_draw(part_splits[5], (N_SEQ * N_REP * POOL_DEV, KVH, PAGE, HD), 1.0, 6.0, ((0, 32), (1, 8)))
    return {"queries": queries, "page_owner": page_owner, "page_slot": page_slot, "lengths": lengths, "keys": keys, "values": values}


masked_score = -1e+30

def reference(queries, page_owner, page_slot, lengths, keys, values):
    request_count = queries.shape[0]
    group_size = QH // KVH
    score_scale = 1.0 / math.sqrt(HD)
    half_index = (jnp.arange(request_count, dtype=jnp.int32) // REQ_DEV % N_REP).astype(jnp.int32)
    page_index = jnp.arange(MAXP, dtype=jnp.int32)
    token_index = jnp.arange(PAGE, dtype=jnp.int32)

    def attend_one(request_data):
        single_query, owner_row, slot_row, token_count, half_side = request_data
        pool_index = ((jnp.maximum(owner_row, 0) * N_REP + half_side) * POOL_DEV + jnp.maximum(slot_row, 0)).astype(jnp.int32)
        page_keys = keys[pool_index].astype(jnp.float32)
        page_values = values[pool_index].astype(jnp.float32)
        grouped_query = single_query.astype(jnp.float32).reshape(KVH, group_size, HD)
        scores = jnp.einsum('kgd,jktd->jkgt', grouped_query, page_keys, precision=lax.Precision.HIGHEST) * score_scale
        live_count = jnp.clip(token_count - page_index * PAGE, 0, PAGE)
        live_tokens = (token_index[None, :] < live_count[:, None])[:, None, None, :]
        scores = jnp.where(live_tokens, scores, masked_score)
        page_max = lax.optimization_barrier(jnp.max(scores, axis=3))
        weights = jnp.where(live_tokens, jnp.exp(scores - page_max[..., None]), 0.0)
        page_sum = lax.optimization_barrier(jnp.sum(weights, axis=3))
        rounded = lax.optimization_barrier(weights.astype(jnp.bfloat16))
        page_out = jnp.einsum('jkgt,jktd->jkgd', rounded.astype(jnp.float32), page_values, precision=lax.Precision.HIGHEST)
        live_pages = (live_count > 0)[:, None, None]
        request_top = lax.optimization_barrier(jnp.max(jnp.where(live_pages, page_max, masked_score), axis=0))
        rescale = jnp.where(live_pages, jnp.exp(jnp.minimum(page_max - request_top[None], 0.0)), 0.0)
        request_total = lax.optimization_barrier(jnp.sum(rescale * page_sum, axis=0))
        request_out = lax.optimization_barrier(jnp.sum(rescale[..., None] * page_out, axis=0))
        return (request_out / request_total[..., None]).astype(jnp.bfloat16).reshape(QH, HD)
    return lax.map(attend_one, (queries, page_owner, page_slot, lengths, half_index))
```

```python
import math

import jax
import jax.numpy as jnp
from jax import lax
from jax.experimental import pallas as pl
from jax.experimental.pallas import tpu as pltpu
from jax.sharding import PartitionSpec as P

masked_score = -1e30
LANES = 128
bf16 = jnp.bfloat16
f32 = jnp.float32
VMEM = pltpu.VMEM


def dot_nt(a, b):
    return lax.dot_general(a, b, (((1,), (1,)), ((), ())), preferred_element_type=f32)


def dot_nn(a, b):
    return lax.dot_general(a, b, (((1,), (0,)), ((), ())), preferred_element_type=f32)


def pieces(x):
    first = x.astype(bf16).astype(f32)
    rest = x - first
    second = rest.astype(bf16).astype(f32)
    third = (rest - second).astype(bf16).astype(f32)
    return first, second, third


def pack_kernel(seq, pool, tokens, q_ref, owner_ref, slot_ref, len_ref, out_ref, q_rows, table):
    rows, heads, width = q_ref.shape
    q_rows[...] = q_ref[...].astype(f32).reshape(rows * heads, width)
    for h in range(heads):
        part = q_rows[pl.ds(h, rows, stride=heads), :]
        many = jnp.concatenate([part] * seq, axis=0).astype(bf16)
        out_ref[:, h * width : (h + 1) * width] = many
    pages = owner_ref.shape[1]
    place = lax.broadcasted_iota(jnp.int32, (1, pages), 1) * tokens
    owner_id = lax.broadcasted_iota(jnp.int32, (seq, pages), 0)
    slot_id = lax.broadcasted_iota(jnp.int32, (LANES, pages), 0)
    for r in range(rows):
        live = jnp.clip(len_ref[r] - place, 0, tokens).astype(f32)
        at = jnp.where(owner_ref[r : r + 1, :] == owner_id, live, 0.0).astype(bf16)
        slot = jnp.where(slot_ref[r : r + 1, :] == slot_id, 1.0, 0.0).astype(bf16)
        table[pl.ds(r, seq, stride=rows), :] = dot_nt(at, slot)
    out_ref[:, heads * width :] = table[...].astype(bf16)


def pages_kernel(pool, heads, in_ref, k_ref, v_ref, out_ref, qs, sc, po):
    width = k_ref.shape[2]
    tokens = k_ref.shape[1]
    reqs = in_ref.shape[0]
    live_of = in_ref[:, heads * width :].astype(f32)
    live_by_page = live_of.T[:pool, :]
    linked_t = live_by_page > 0.0
    live = jnp.max(live_by_page, axis=1, keepdims=True)
    picker = jnp.where(linked_t, 1.0, 0.0).astype(bf16)
    slot_q = dot_nn(picker, in_ref[:, : heads * width])
    for h in range(heads):
        qs[pl.ds(h, pool, stride=heads), :] = slot_q[:, h * width : (h + 1) * width]
    for p in range(pool):
        rows = slice(p * heads, (p + 1) * heads)
        sc[rows, :] = dot_nt(qs[rows, :].astype(bf16), k_ref[p])
    scale = 1.0 / math.sqrt(width)
    mask = lax.broadcasted_iota(jnp.int32, (pool, tokens), 1).astype(f32) < live
    page_max, page_sum = [], []
    for h in range(heads):
        rows = pl.ds(h, pool, stride=heads)
        s = jnp.where(mask, sc[rows, :] * scale, masked_score)
        m = jnp.max(s, axis=1, keepdims=True)
        w = jnp.where(mask, jnp.exp(s - m), 0.0)
        sc[rows, :] = w
        page_max.append(m)
        page_sum.append(jnp.sum(w, axis=1, keepdims=True))
    for p in range(pool):
        rows = slice(p * heads, (p + 1) * heads)
        po[rows, :] = dot_nn(sc[rows, :].astype(bf16), v_ref[p])
    tops, sums, scaled = [], [], []
    for h in range(heads):
        top = jnp.max(jnp.where(linked_t, page_max[h], masked_score), axis=0, keepdims=True)
        page_top = jnp.max(jnp.where(linked_t, top, masked_score), axis=1, keepdims=True)
        rescale = jnp.exp(jnp.minimum(page_max[h] - page_top, 0.0))
        tops.append(top)
        sums.append(
            jnp.sum(jnp.where(linked_t, page_sum[h] * rescale, 0.0), axis=0, keepdims=True)
        )
        scaled.append(po[pl.ds(h, pool, stride=heads), :] * rescale)
    top = jnp.concatenate(tops, axis=0)
    total = jnp.concatenate(sums, axis=0)
    inverse = jnp.where(total > 0.0, 1.0 / jnp.where(total > 0.0, total, 1.0), 0.0)
    m1, m2, m3 = pieces(top)
    s1, s2, s3 = pieces(total)
    filler = jnp.zeros((LANES - 7 * heads, reqs), f32)
    stats = jnp.concatenate([m1, m2, m3, s1, s2, s3, inverse, filler], axis=0).T
    out_ref[:, heads * width :] = stats.astype(bf16)
    linked = jnp.where(live_of[:, :pool] > 0.0, 1.0, 0.0).astype(bf16)
    linked3 = jnp.concatenate([linked] * 3, axis=1)
    for h in range(heads):
        stack = jnp.concatenate(pieces(scaled[h]), axis=0).astype(bf16)
        joined = dot_nn(linked3, stack)
        joined = joined * stats[:, 6 * heads + h : 6 * heads + h + 1]
        out_ref[:, h * width : (h + 1) * width] = joined.astype(bf16)


def merge_kernel(heads, rows, in_ref, out_ref, scratch):
    width = out_ref.shape[1]
    reqs = in_ref.shape[0]
    stats = in_ref[:, heads * width :].astype(f32).T
    part = [stats[k * heads : (k + 1) * heads, :] for k in range(6)]
    top = part[0] + part[1] + part[2]
    total = part[3] + part[4] + part[5]
    overall = top
    step = rows
    while step < reqs:
        overall = jnp.maximum(overall, pltpu.roll(overall, step, 1))
        step *= 2
    share = jnp.exp(top - overall) * total
    whole = share
    step = rows
    while step < reqs:
        whole = whole + pltpu.roll(whole, step, 1)
        step *= 2
    share = share / whole
    filler = jnp.zeros((LANES - heads, reqs), f32)
    share = jnp.concatenate([share, filler], axis=0).T
    for h in range(heads):
        x = in_ref[:, h * width : (h + 1) * width].astype(f32) * share[:, h : h + 1]
        x = jnp.sum(x.reshape(reqs // rows, rows, width), axis=0)
        scratch[pl.ds(h, rows, stride=heads), :] = x
    out_ref[...] = scratch[...].astype(bf16)


def on_device(queries, page_owner, page_slot, lengths, keys, values):
    rows, heads, width = queries.shape
    pool, _, tokens, _ = keys.shape
    seq = lax.axis_size("seq")
    reqs = seq * rows
    row_width = heads * width + LANES
    whole = pl.BlockSpec(memory_space=VMEM)
    packed = pl.pallas_call(
        lambda *refs: pack_kernel(seq, pool, tokens, *refs),
        out_shape=jax.ShapeDtypeStruct((reqs, row_width), bf16),
        in_specs=[whole, whole, whole, pl.BlockSpec(memory_space=pltpu.SMEM)],
        out_specs=whole,
        scratch_shapes=[VMEM((rows * heads, width), f32), VMEM((reqs, LANES), f32)],
        name="pack",
    )(queries, page_owner, page_slot, lengths)
    got = lax.all_to_all(packed, "seq", 0, 0, tiled=True)
    partial = pl.pallas_call(
        lambda *refs: pages_kernel(pool, heads, *refs),
        out_shape=jax.ShapeDtypeStruct((reqs, row_width), bf16),
        in_specs=[whole, whole, whole],
        out_specs=whole,
        scratch_shapes=[VMEM((pool * heads, width), f32)] * 3,
        name="pages",
    )(got, keys.reshape(pool, tokens, width), values.reshape(pool, tokens, width))
    back = lax.all_to_all(partial, "seq", 0, 0, tiled=True)
    out = pl.pallas_call(
        lambda *refs: merge_kernel(heads, rows, *refs),
        out_shape=jax.ShapeDtypeStruct((rows * heads, width), bf16),
        in_specs=[whole],
        out_specs=whole,
        scratch_shapes=[VMEM((rows * heads, width), f32)],
        name="merge",
    )(back)
    return out.reshape(rows, heads, width)


def solution(mesh):
    placed = (
        P(("groups", "seq", "rep"), "head", None),
        P(("groups", "seq", "rep"), None),
        P(("groups", "seq", "rep"), None),
        P(("groups", "seq", "rep")),
        P(("groups", "seq", "rep"), "head", None, None),
        P(("groups", "seq", "rep"), "head", None, None),
    )
    return jax.shard_map(
        on_device,
        mesh=mesh,
        in_specs=placed,
        out_specs=P(("groups", "seq", "rep"), "head", None),
        check_vma=False,
    )
```

```python
import math

import jax
import jax.numpy as jnp
from jax import lax
from jax.experimental import pallas as pl
from jax.experimental.pallas import tpu as pltpu
from jax.sharding import PartitionSpec as P

masked_score = -1e30
LANES = 128
bf16 = jnp.bfloat16
f32 = jnp.float32
VMEM = pltpu.VMEM


def dot_nt(a, b):
    return lax.dot_general(a, b, (((1,), (1,)), ((), ())), preferred_element_type=f32)


def dot_nn(a, b):
    return lax.dot_general(a, b, (((1,), (0,)), ((), ())), preferred_element_type=f32)


def pieces(x):
    first = x.astype(bf16).astype(f32)
    rest = x - first
    second = rest.astype(bf16).astype(f32)
    third = (rest - second).astype(bf16).astype(f32)
    return first, second, third


def pack_kernel(seq, tokens, q_hbm, owner_hbm, slot_hbm, len_hbm, out_ref, *scratch):
    q_ref, owner_ref, slot_ref, len_ref, sems, q_rows, table = scratch
    pairs = (len_hbm, len_ref), (owner_hbm, owner_ref), (slot_hbm, slot_ref), (q_hbm, q_ref)
    loads = [pltpu.make_async_copy(a, b, sems.at[i]) for i, (a, b) in enumerate(pairs)]
    for load in loads:
        load.start()
    rows, heads, width = q_ref.shape
    for load in loads[:3]:
        load.wait()
    pages = owner_ref.shape[1]
    place = lax.broadcasted_iota(jnp.int32, (1, pages), 1) * tokens
    owner_id = lax.broadcasted_iota(jnp.int32, (seq, pages), 0)
    slot_id = lax.broadcasted_iota(jnp.int32, (LANES, pages), 0)
    for r in range(rows):
        live = jnp.clip(len_ref[r] - place, 0, tokens).astype(f32)
        at = jnp.where(owner_ref[r : r + 1, :] == owner_id, live, 0.0).astype(bf16)
        slot = jnp.where(slot_ref[r : r + 1, :] == slot_id, 1.0, 0.0).astype(bf16)
        table[pl.ds(r, seq, stride=rows), :] = dot_nt(at, slot)
    out_ref[:, heads * width :] = table[...].astype(bf16)
    loads[3].wait()
    q_rows[...] = q_ref[...].astype(f32).reshape(rows * heads, width)
    for h in range(heads):
        part = q_rows[pl.ds(h, rows, stride=heads), :]
        many = jnp.concatenate([part] * seq, axis=0).astype(bf16)
        out_ref[:, h * width : (h + 1) * width] = many


def pages_kernel(pool, heads, in_ref, k_ref, v_ref, out_ref, qs, sc, po):
    width = k_ref.shape[2]
    tokens = k_ref.shape[1]
    reqs = in_ref.shape[0]
    live_of = in_ref[:, heads * width :].astype(f32)
    live_by_page = live_of.T[:pool, :]
    linked_t = live_by_page > 0.0
    live = jnp.max(live_by_page, axis=1, keepdims=True)
    picker = jnp.where(linked_t, 1.0, 0.0).astype(bf16)
    slot_q = dot_nn(picker, in_ref[:, : heads * width])
    for h in range(heads):
        qs[pl.ds(h, pool, stride=heads), :] = slot_q[:, h * width : (h + 1) * width]
    for p in range(pool):
        rows = slice(p * heads, (p + 1) * heads)
        sc[rows, :] = dot_nt(qs[rows, :].astype(bf16), k_ref[p])
    scale = 1.0 / math.sqrt(width)
    mask = lax.broadcasted_iota(jnp.int32, (pool, tokens), 1).astype(f32) < live
    page_max, page_sum = [], []
    for h in range(heads):
        rows = pl.ds(h, pool, stride=heads)
        s = jnp.where(mask, sc[rows, :] * scale, masked_score)
        m = jnp.max(s, axis=1, keepdims=True)
        w = jnp.where(mask, jnp.exp(s - m), 0.0)
        sc[rows, :] = w
        page_max.append(m)
        page_sum.append(jnp.sum(w, axis=1, keepdims=True))
    for p in range(pool):
        rows = slice(p * heads, (p + 1) * heads)
        po[rows, :] = dot_nn(sc[rows, :].astype(bf16), v_ref[p])
    tops, sums, scaled = [], [], []
    for h in range(heads):
        top = jnp.max(jnp.where(linked_t, page_max[h], masked_score), axis=0, keepdims=True)
        page_top = jnp.max(jnp.where(linked_t, top, masked_score), axis=1, keepdims=True)
        rescale = jnp.exp(jnp.minimum(page_max[h] - page_top, 0.0))
        tops.append(top)
        sums.append(
            jnp.sum(jnp.where(linked_t, page_sum[h] * rescale, 0.0), axis=0, keepdims=True)
        )
        scaled.append(po[pl.ds(h, pool, stride=heads), :] * rescale)
    top = jnp.concatenate(tops, axis=0)
    total = jnp.concatenate(sums, axis=0)
    inverse = jnp.where(total > 0.0, 1.0 / jnp.where(total > 0.0, total, 1.0), 0.0)
    m1, m2, m3 = pieces(top)
    s1, s2, s3 = pieces(total)
    filler = jnp.zeros((LANES - 7 * heads, reqs), f32)
    stats = jnp.concatenate([m1, m2, m3, s1, s2, s3, inverse, filler], axis=0).T
    out_ref[:, heads * width :] = stats.astype(bf16)
    linked = jnp.where(live_of[:, :pool] > 0.0, 1.0, 0.0).astype(bf16)
    linked3 = jnp.concatenate([linked] * 3, axis=1)
    for h in range(heads):
        stack = jnp.concatenate(pieces(scaled[h]), axis=0).astype(bf16)
        joined = dot_nn(linked3, stack)
        joined = joined * stats[:, 6 * heads + h : 6 * heads + h + 1]
        out_ref[:, h * width : (h + 1) * width] = joined.astype(bf16)


def merge_kernel(heads, rows, in_ref, out_ref, scratch):
    width = out_ref.shape[1]
    reqs = in_ref.shape[0]
    stats = in_ref[:, heads * width :].astype(f32).T
    part = [stats[k * heads : (k + 1) * heads, :] for k in range(6)]
    top = part[0] + part[1] + part[2]
    total = part[3] + part[4] + part[5]
    overall = top
    step = rows
    while step < reqs:
        overall = jnp.maximum(overall, pltpu.roll(overall, step, 1))
        step *= 2
    share = jnp.exp(top - overall) * total
    whole = share
    step = rows
    while step < reqs:
        whole = whole + pltpu.roll(whole, step, 1)
        step *= 2
    share = share / whole
    filler = jnp.zeros((LANES - heads, reqs), f32)
    share = jnp.concatenate([share, filler], axis=0).T
    for h in range(heads):
        x = in_ref[:, h * width : (h + 1) * width].astype(f32) * share[:, h : h + 1]
        x = jnp.sum(x.reshape(reqs // rows, rows, width), axis=0)
        scratch[pl.ds(h, rows, stride=heads), :] = x
    out_ref[...] = scratch[...].astype(bf16)


def on_device(queries, page_owner, page_slot, lengths, keys, values):
    rows, heads, width = queries.shape
    pool, _, tokens, _ = keys.shape
    seq = lax.axis_size("seq")
    reqs = seq * rows
    row_width = heads * width + LANES
    whole = pl.BlockSpec(memory_space=VMEM)
    hbm = pl.BlockSpec(memory_space=pltpu.HBM)
    small = (queries, page_owner, page_slot, lengths)
    packed = pl.pallas_call(
        lambda *refs: pack_kernel(seq, tokens, *refs),
        out_shape=jax.ShapeDtypeStruct((reqs, row_width), bf16),
        in_specs=[hbm] * 4,
        out_specs=whole,
        scratch_shapes=[
            VMEM(queries.shape, bf16),
            VMEM(page_owner.shape, jnp.int32),
            VMEM(page_slot.shape, jnp.int32),
            pltpu.SMEM(lengths.shape, jnp.int32),
            pltpu.SemaphoreType.DMA((4,)),
            VMEM((rows * heads, width), f32),
            VMEM((reqs, LANES), f32),
        ],
        cost_estimate=pl.CostEstimate(flops=1 << 33, bytes_accessed=1 << 19, transcendentals=0),
        compiler_params=pltpu.CompilerParams(vmem_limit_bytes=4 << 20),
        name="pack",
    )(*[pltpu.with_memory_space_constraint(a, pltpu.HBM) for a in small])
    got = lax.all_to_all(packed, "seq", 0, 0, tiled=True)
    partial = pl.pallas_call(
        lambda *refs: pages_kernel(pool, heads, *refs),
        out_shape=jax.ShapeDtypeStruct((reqs, row_width), bf16),
        in_specs=[whole, whole, whole],
        out_specs=whole,
        scratch_shapes=[VMEM((pool * heads, width), f32)] * 3,
        compiler_params=pltpu.CompilerParams(vmem_limit_bytes=12 << 20),
        name="pages",
    )(got, keys.reshape(pool, tokens, width), values.reshape(pool, tokens, width))
    back = lax.all_to_all(partial, "seq", 0, 0, tiled=True)
    out = pl.pallas_call(
        lambda *refs: merge_kernel(heads, rows, *refs),
        out_shape=jax.ShapeDtypeStruct((rows * heads, width), bf16),
        in_specs=[whole],
        out_specs=whole,
        scratch_shapes=[VMEM((rows * heads, width), f32)],
        compiler_params=pltpu.CompilerParams(vmem_limit_bytes=4 << 20),
        name="merge",
    )(back)
    return out.reshape(rows, heads, width)


def solution(mesh):
    placed = (
        P(("groups", "seq", "rep"), "head", None),
        P(("groups", "seq", "rep"), None),
        P(("groups", "seq", "rep"), None),
        P(("groups", "seq", "rep")),
        P(("groups", "seq", "rep"), "head", None, None),
        P(("groups", "seq", "rep"), "head", None, None),
    )
    return jax.shard_map(
        on_device,
        mesh=mesh,
        in_specs=placed,
        out_specs=P(("groups", "seq", "rep"), "head", None),
        check_vma=False,
    )
```

```python
import math

import jax
import jax.numpy as jnp
from jax import lax
from jax.experimental import pallas as pl
from jax.experimental.pallas import tpu as pltpu
from jax.sharding import PartitionSpec as P

masked_score = -1e30
LANES = 128
STAGGER_NS = 6000
bf16 = jnp.bfloat16
f32 = jnp.float32
VMEM = pltpu.VMEM


def dot_nt(a, b):
    return lax.dot_general(a, b, (((1,), (1,)), ((), ())), preferred_element_type=f32)


def dot_nn(a, b):
    return lax.dot_general(a, b, (((1,), (0,)), ((), ())), preferred_element_type=f32)


def pieces(x):
    first = x.astype(bf16).astype(f32)
    rest = x - first
    second = rest.astype(bf16).astype(f32)
    third = (rest - second).astype(bf16).astype(f32)
    return first, second, third


def pack_kernel(seq, tokens, q_hbm, owner_hbm, slot_hbm, len_hbm, out_ref, *scratch):
    q_ref, owner_ref, slot_ref, len_ref, sems, q_rows, table = scratch
    pairs = (len_hbm, len_ref), (owner_hbm, owner_ref), (slot_hbm, slot_ref), (q_hbm, q_ref)
    loads = [pltpu.make_async_copy(a, b, sems.at[i]) for i, (a, b) in enumerate(pairs)]
    for load in loads:
        load.start()
    rows, heads, width = q_ref.shape
    for load in loads[:3]:
        load.wait()
    pages = owner_ref.shape[1]
    place = lax.broadcasted_iota(jnp.int32, (1, pages), 1) * tokens
    owner_id = lax.broadcasted_iota(jnp.int32, (seq, pages), 0)
    slot_id = lax.broadcasted_iota(jnp.int32, (LANES, pages), 0)
    for r in range(rows):
        live = jnp.clip(len_ref[r] - place, 0, tokens).astype(f32)
        at = jnp.where(owner_ref[r : r + 1, :] == owner_id, live, 0.0).astype(bf16)
        slot = jnp.where(slot_ref[r : r + 1, :] == slot_id, 1.0, 0.0).astype(bf16)
        table[pl.ds(r, seq, stride=rows), :] = dot_nt(at, slot)
    out_ref[:, heads * width :] = table[...].astype(bf16)

    @pl.when(lax.axis_index("rep") == 0)
    def _():
        pl.delay(STAGGER_NS)

    loads[3].wait()
    q_rows[...] = q_ref[...].astype(f32).reshape(rows * heads, width)
    for h in range(heads):
        part = q_rows[pl.ds(h, rows, stride=heads), :]
        many = jnp.concatenate([part] * seq, axis=0).astype(bf16)
        out_ref[:, h * width : (h + 1) * width] = many


def pages_kernel(pool, heads, in_ref, k_ref, v_ref, out_ref, qs, sc, po):
    width = k_ref.shape[2]
    tokens = k_ref.shape[1]
    reqs = in_ref.shape[0]
    live_of = in_ref[:, heads * width :].astype(f32)
    live_by_page = live_of.T[:pool, :]
    linked_t = live_by_page > 0.0
    live = jnp.max(live_by_page, axis=1, keepdims=True)
    picker = jnp.where(linked_t, 1.0, 0.0).astype(bf16)
    slot_q = dot_nn(picker, in_ref[:, : heads * width])
    for h in range(heads):
        qs[pl.ds(h, pool, stride=heads), :] = slot_q[:, h * width : (h + 1) * width]
    for p in range(pool):
        rows = slice(p * heads, (p + 1) * heads)
        sc[rows, :] = dot_nt(qs[rows, :].astype(bf16), k_ref[p])
    scale = 1.0 / math.sqrt(width)
    mask = lax.broadcasted_iota(jnp.int32, (pool, tokens), 1).astype(f32) < live
    page_max, page_sum = [], []
    for h in range(heads):
        rows = pl.ds(h, pool, stride=heads)
        s = jnp.where(mask, sc[rows, :] * scale, masked_score)
        m = jnp.max(s, axis=1, keepdims=True)
        w = jnp.where(mask, jnp.exp(s - m), 0.0)
        sc[rows, :] = w
        page_max.append(m)
        page_sum.append(jnp.sum(w, axis=1, keepdims=True))
    for p in range(pool):
        rows = slice(p * heads, (p + 1) * heads)
        po[rows, :] = dot_nn(sc[rows, :].astype(bf16), v_ref[p])
    tops, sums, scaled = [], [], []
    for h in range(heads):
        top = jnp.max(jnp.where(linked_t, page_max[h], masked_score), axis=0, keepdims=True)
        page_top = jnp.max(jnp.where(linked_t, top, masked_score), axis=1, keepdims=True)
        rescale = jnp.exp(jnp.minimum(page_max[h] - page_top, 0.0))
        tops.append(top)
        sums.append(
            jnp.sum(jnp.where(linked_t, page_sum[h] * rescale, 0.0), axis=0, keepdims=True)
        )
        scaled.append(po[pl.ds(h, pool, stride=heads), :] * rescale)
    top = jnp.concatenate(tops, axis=0)
    total = jnp.concatenate(sums, axis=0)
    inverse = jnp.where(total > 0.0, 1.0 / jnp.where(total > 0.0, total, 1.0), 0.0)
    m1, m2, m3 = pieces(top)
    s1, s2, s3 = pieces(total)
    filler = jnp.zeros((LANES - 7 * heads, reqs), f32)
    stats = jnp.concatenate([m1, m2, m3, s1, s2, s3, inverse, filler], axis=0).T
    out_ref[:, heads * width :] = stats.astype(bf16)
    linked = jnp.where(live_of[:, :pool] > 0.0, 1.0, 0.0).astype(bf16)
    linked3 = jnp.concatenate([linked] * 3, axis=1)
    for h in range(heads):
        stack = jnp.concatenate(pieces(scaled[h]), axis=0).astype(bf16)
        joined = dot_nn(linked3, stack)
        joined = joined * stats[:, 6 * heads + h : 6 * heads + h + 1]
        out_ref[:, h * width : (h + 1) * width] = joined.astype(bf16)


def merge_kernel(heads, rows, in_ref, out_ref, scratch):
    width = out_ref.shape[1]
    reqs = in_ref.shape[0]
    stats = in_ref[:, heads * width :].astype(f32)

    def lanes_from(x, at):
        return pltpu.roll(x, LANES - at, 1)

    joined = stats + lanes_from(stats, heads) + lanes_from(stats, 2 * heads)
    by_source = (reqs // rows, rows, LANES)
    top = joined.reshape(by_source)
    total = lanes_from(joined, 3 * heads).reshape(by_source)
    share = jnp.exp(top - jnp.max(top, axis=0, keepdims=True)) * total
    share = share * (1.0 / jnp.sum(share, axis=0, keepdims=True))
    share = share.reshape(reqs, LANES)
    for h in range(heads):
        x = in_ref[:, h * width : (h + 1) * width].astype(f32) * share[:, h : h + 1]
        x = jnp.sum(x.reshape(reqs // rows, rows, width), axis=0)
        scratch[pl.ds(h, rows, stride=heads), :] = x
    out_ref[...] = scratch[...].astype(bf16)


def on_device(queries, page_owner, page_slot, lengths, keys, values):
    rows, heads, width = queries.shape
    pool, _, tokens, _ = keys.shape
    seq = lax.axis_size("seq")
    reqs = seq * rows
    row_width = heads * width + LANES
    whole = pl.BlockSpec(memory_space=VMEM)
    hbm = pl.BlockSpec(memory_space=pltpu.HBM)
    small = (queries, page_owner, page_slot, lengths)
    packed = pl.pallas_call(
        lambda *refs: pack_kernel(seq, tokens, *refs),
        out_shape=jax.ShapeDtypeStruct((reqs, row_width), bf16),
        in_specs=[hbm] * 4,
        out_specs=whole,
        scratch_shapes=[
            VMEM(queries.shape, bf16),
            VMEM(page_owner.shape, jnp.int32),
            VMEM(page_slot.shape, jnp.int32),
            pltpu.SMEM(lengths.shape, jnp.int32),
            pltpu.SemaphoreType.DMA((4,)),
            VMEM((rows * heads, width), f32),
            VMEM((reqs, LANES), f32),
        ],
        cost_estimate=pl.CostEstimate(flops=1 << 33, bytes_accessed=1 << 19, transcendentals=0),
        compiler_params=pltpu.CompilerParams(vmem_limit_bytes=4 << 20),
        name="pack",
    )(*[pltpu.with_memory_space_constraint(a, pltpu.HBM) for a in small])
    got = lax.all_to_all(packed, "seq", 0, 0, tiled=True)
    partial = pl.pallas_call(
        lambda *refs: pages_kernel(pool, heads, *refs),
        out_shape=jax.ShapeDtypeStruct((reqs, row_width), bf16),
        in_specs=[whole, whole, whole],
        out_specs=whole,
        scratch_shapes=[VMEM((pool * heads, width), f32)] * 3,
        compiler_params=pltpu.CompilerParams(vmem_limit_bytes=12 << 20),
        name="pages",
    )(got, keys.reshape(pool, tokens, width), values.reshape(pool, tokens, width))
    back = lax.all_to_all(partial, "seq", 0, 0, tiled=True)
    out = pl.pallas_call(
        lambda *refs: merge_kernel(heads, rows, *refs),
        out_shape=jax.ShapeDtypeStruct((rows * heads, width), bf16),
        in_specs=[whole],
        out_specs=whole,
        scratch_shapes=[VMEM((rows * heads, width), f32)],
        compiler_params=pltpu.CompilerParams(vmem_limit_bytes=4 << 20),
        name="merge",
    )(back)
    return out.reshape(rows, heads, width)


def solution(mesh):
    placed = (
        P(("groups", "seq", "rep"), "head", None),
        P(("groups", "seq", "rep"), None),
        P(("groups", "seq", "rep"), None),
        P(("groups", "seq", "rep")),
        P(("groups", "seq", "rep"), "head", None, None),
        P(("groups", "seq", "rep"), "head", None, None),
    )
    return jax.shard_map(
        on_device,
        mesh=mesh,
        in_specs=placed,
        out_specs=P(("groups", "seq", "rep"), "head", None),
        check_vma=False,
    )
```

```python
import math

import jax
import jax.numpy as jnp
from jax import lax
from jax.experimental import pallas as pl
from jax.experimental.pallas import tpu as pltpu
from jax.sharding import PartitionSpec as P

masked_score = -1e30
LANES = 128
PIECES = 3
STAGGER_NS = 5000
bf16 = jnp.bfloat16
f32 = jnp.float32
VMEM = pltpu.VMEM


def dot_nt(a, b):
    return lax.dot_general(a, b, (((1,), (1,)), ((), ())), preferred_element_type=f32)


def dot_nn(a, b):
    return lax.dot_general(a, b, (((1,), (0,)), ((), ())), preferred_element_type=f32)


def pieces(x):
    first = x.astype(bf16).astype(f32)
    rest = x - first
    second = rest.astype(bf16).astype(f32)
    third = (rest - second).astype(bf16).astype(f32)
    return first, second, third


def chunk_rows(d, h, rows, heads):
    at = d * (rows * heads + rows // 2) + h * rows
    return slice(at, at + rows)


def fold(ref, x, rows, heads):
    half = rows // 2
    for d in range(x.shape[0] // rows):
        piece = x[d * rows : (d + 1) * rows, :]
        other = pltpu.roll(pltpu.roll(piece, half, 0), LANES // 2, 1)
        at = chunk_rows(d, heads, rows, heads).start
        ref[at : at + half, :] = (piece + other)[:half, :].astype(bf16)


def unfold(ref, rows, heads):
    half = rows // 2
    out = []
    for d in range(ref.shape[0] // (rows * heads + half)):
        at = chunk_rows(d, heads, rows, heads).start
        piece = ref[at : at + half, :].astype(f32)
        out += [piece, pltpu.roll(piece, LANES // 2, 1)]
    return jnp.concatenate(out, axis=0)


def pack_kernel(seq, tokens, q_hbm, owner_hbm, slot_hbm, len_hbm, out_ref, *scratch):
    q_ref, owner_ref, slot_ref, len_ref, sems, q_rows, table = scratch
    pairs = (len_hbm, len_ref), (owner_hbm, owner_ref), (slot_hbm, slot_ref), (q_hbm, q_ref)
    loads = [pltpu.make_async_copy(a, b, sems.at[i]) for i, (a, b) in enumerate(pairs)]
    for load in loads:
        load.start()
    rows, heads, width = q_ref.shape
    for load in loads[:3]:
        load.wait()
    pages = owner_ref.shape[1]
    place = lax.broadcasted_iota(jnp.int32, (1, pages), 1) * tokens
    owner_id = lax.broadcasted_iota(jnp.int32, (seq, pages), 0)
    slot_id = lax.broadcasted_iota(jnp.int32, (LANES, pages), 0)
    for r in range(rows):
        live = jnp.clip(len_ref[r] - place, 0, tokens).astype(f32)
        at = jnp.where(owner_ref[r : r + 1, :] == owner_id, live, 0.0).astype(bf16)
        slot = jnp.where(slot_ref[r : r + 1, :] == slot_id, 1.0, 0.0).astype(bf16)
        table[pl.ds(r, seq, stride=rows), :] = dot_nt(at, slot)
    fold(out_ref, table[...], rows, heads)

    @pl.when(lax.axis_index("rep") == 0)
    def _():
        pl.delay(STAGGER_NS)

    loads[3].wait()
    q_rows[...] = q_ref[...].astype(f32).reshape(rows * heads, width)
    for h in range(heads):
        part = q_rows[pl.ds(h, rows, stride=heads), :]
        part = part.astype(bf16)
        for d in range(seq):
            out_ref[chunk_rows(d, h, rows, heads), :] = part


def side_by_side(ref, p, heads):
    first = ref[p * heads : (p + 1) * heads, :]
    second = ref[(p + 1) * heads : (p + 2) * heads, :]
    none = jnp.zeros_like(first)
    left = jnp.concatenate([first, none], axis=0)
    right = jnp.concatenate([none, second], axis=0)
    return jnp.concatenate([left, right], axis=1).astype(bf16)


def pages_kernel(pool, heads, rows, in_ref, k_ref, v_ref, out_ref, qs, sc, po):
    width = k_ref.shape[2]
    tokens = k_ref.shape[1]
    live_of = unfold(in_ref, rows, heads)
    reqs = live_of.shape[0]
    live_by_page = live_of.T[:pool, :]
    linked_t = live_by_page > 0.0
    live = jnp.max(live_by_page, axis=1, keepdims=True)
    picker = jnp.where(linked_t, 1.0, 0.0).astype(bf16)
    seq = reqs // rows
    for h in range(0, heads, 2):
        asked = [
            jnp.concatenate(
                [in_ref[chunk_rows(d, h + i, rows, heads), :].astype(f32) for d in range(seq)], axis=0
            )
            for i in range(2)
        ]
        slot_q = dot_nn(picker, jnp.concatenate(asked, axis=1).astype(bf16))
        for i in range(2):
            qs[pl.ds(h + i, pool, stride=heads), :] = slot_q[:, i * width : (i + 1) * width]
    for p in range(0, pool, 2):
        both = jnp.concatenate([k_ref[p], k_ref[p + 1]], axis=1)
        sc[p * heads : (p + 2) * heads, :] = dot_nt(side_by_side(qs, p, heads), both)
    scale = 1.0 / math.sqrt(width)
    mask = lax.broadcasted_iota(jnp.int32, (pool, tokens), 1).astype(f32) < live
    page_max, page_sum = [], []
    for h in range(heads):
        of_head = pl.ds(h, pool, stride=heads)
        s = jnp.where(mask, sc[of_head, :] * scale, masked_score)
        m = jnp.max(s, axis=1, keepdims=True)
        w = jnp.where(mask, jnp.exp(s - m), 0.0)
        sc[of_head, :] = w
        page_max.append(m)
        page_sum.append(jnp.sum(w, axis=1, keepdims=True))
    for p in range(0, pool, 2):
        both = v_ref[p : p + 2].reshape(2 * tokens, width)
        po[p * heads : (p + 2) * heads, :] = dot_nn(side_by_side(sc, p, heads), both)
    tops, sums, scaled = [], [], []
    for h in range(heads):
        top = jnp.max(jnp.where(linked_t, page_max[h], masked_score), axis=0, keepdims=True)
        page_top = jnp.max(jnp.where(linked_t, top, masked_score), axis=1, keepdims=True)
        rescale = jnp.exp(jnp.minimum(page_max[h] - page_top, 0.0))
        tops.append(top)
        sums.append(
            jnp.sum(jnp.where(linked_t, page_sum[h] * rescale, 0.0), axis=0, keepdims=True)
        )
        scaled.append(po[pl.ds(h, pool, stride=heads), :] * rescale)
    top = jnp.concatenate(tops, axis=0)
    total = jnp.concatenate(sums, axis=0)
    inverse = jnp.where(total > 0.0, 1.0 / jnp.where(total > 0.0, total, 1.0), 0.0)
    m1, m2, m3 = pieces(top)
    s1, s2, s3 = pieces(total)
    filler = jnp.zeros((LANES - 7 * heads, reqs), f32)
    stats = jnp.concatenate([m1, m2, m3, s1, s2, s3, inverse, filler], axis=0).T
    fold(out_ref, stats, rows, heads)
    linked = jnp.where(live_of[:, :pool] > 0.0, 1.0, 0.0).astype(bf16)
    linked = jnp.concatenate([linked] * PIECES, axis=1)
    for h in range(0, heads, 2):
        stack = [jnp.concatenate(pieces(x)[:PIECES], axis=0) for x in scaled[h : h + 2]]
        both = dot_nn(linked, jnp.concatenate(stack, axis=1).astype(bf16))
        for i in range(2):
            joined = both[:, i * width : (i + 1) * width]
            joined = joined * stats[:, 6 * heads + h + i : 6 * heads + h + i + 1]
            for d in range(seq):
                piece = joined[d * rows : (d + 1) * rows, :].astype(bf16)
                out_ref[chunk_rows(d, h + i, rows, heads), :] = piece


def merge_kernel(heads, rows, in_ref, out_ref, scratch):
    stats = unfold(in_ref, rows, heads)
    reqs = stats.shape[0]

    def lanes_from(x, at):
        return pltpu.roll(x, LANES - at, 1)

    joined = stats + lanes_from(stats, heads) + lanes_from(stats, 2 * heads)
    by_source = (reqs // rows, rows, LANES)
    top = joined.reshape(by_source)
    total = lanes_from(joined, 3 * heads).reshape(by_source)
    share = jnp.exp(top - jnp.max(top, axis=0, keepdims=True)) * total
    share = share * (1.0 / jnp.sum(share, axis=0, keepdims=True))
    share = share.reshape(reqs, LANES)
    for h in range(heads):
        total = None
        for d in range(reqs // rows):
            x = in_ref[chunk_rows(d, h, rows, heads), :].astype(f32)
            x = x * share[d * rows : (d + 1) * rows, h : h + 1]
            total = x if total is None else total + x
        scratch[pl.ds(h, rows, stride=heads), :] = total
    out_ref[...] = scratch[...].astype(bf16)


def on_device(queries, page_owner, page_slot, lengths, keys, values):
    rows, heads, width = queries.shape
    pool, _, tokens, _ = keys.shape
    seq = lax.axis_size("seq")
    reqs = seq * rows
    chunk = rows * heads + rows // 2
    whole = pl.BlockSpec(memory_space=VMEM)
    hbm = pl.BlockSpec(memory_space=pltpu.HBM)
    small = (queries, page_owner, page_slot, lengths)
    packed = pl.pallas_call(
        lambda *refs: pack_kernel(seq, tokens, *refs),
        out_shape=jax.ShapeDtypeStruct((seq * chunk, width), bf16),
        in_specs=[hbm] * 4,
        out_specs=whole,
        scratch_shapes=[
            VMEM(queries.shape, bf16),
            VMEM(page_owner.shape, jnp.int32),
            VMEM(page_slot.shape, jnp.int32),
            pltpu.SMEM(lengths.shape, jnp.int32),
            pltpu.SemaphoreType.DMA((4,)),
            VMEM((rows * heads, width), f32),
            VMEM((reqs, LANES), f32),
        ],
        cost_estimate=pl.CostEstimate(flops=1 << 33, bytes_accessed=1 << 19, transcendentals=0),
        compiler_params=pltpu.CompilerParams(vmem_limit_bytes=4 << 20),
        name="pack",
    )(*[pltpu.with_memory_space_constraint(a, pltpu.HBM) for a in small])

    def exchange(x):
        x = x.reshape(seq, 2 * chunk // rows, rows // 2, width)
        return lax.all_to_all(x, "seq", 0, 0, tiled=True).reshape(seq * chunk, width)

    got = exchange(packed)
    partial = pl.pallas_call(
        lambda *refs: pages_kernel(pool, heads, rows, *refs),
        out_shape=jax.ShapeDtypeStruct((seq * chunk, width), bf16),
        in_specs=[whole, whole, whole],
        out_specs=whole,
        scratch_shapes=[VMEM((pool * heads, width), f32)] * 3,
        compiler_params=pltpu.CompilerParams(vmem_limit_bytes=12 << 20),
        name="pages",
    )(got, keys.reshape(pool, tokens, width), values.reshape(pool, tokens, width))
    back = exchange(partial)
    out = pl.pallas_call(
        lambda *refs: merge_kernel(heads, rows, *refs),
        out_shape=jax.ShapeDtypeStruct((rows * heads, width), bf16),
        in_specs=[whole],
        out_specs=whole,
        scratch_shapes=[VMEM((rows * heads, width), f32)],
        compiler_params=pltpu.CompilerParams(vmem_limit_bytes=4 << 20),
        name="merge",
    )(back)
    return out.reshape(rows, heads, width)


def solution(mesh):
    placed = (
        P(("groups", "seq", "rep"), "head", None),
        P(("groups", "seq", "rep"), None),
        P(("groups", "seq", "rep"), None),
        P(("groups", "seq", "rep")),
        P(("groups", "seq", "rep"), "head", None, None),
        P(("groups", "seq", "rep"), "head", None, None),
    )
    return jax.shard_map(
        on_device,
        mesh=mesh,
        in_specs=placed,
        out_specs=P(("groups", "seq", "rep"), "head", None),
        check_vma=False,
    )
```

```python
import math

import jax
import jax.numpy as jnp
from jax import lax
from jax.experimental import pallas as pl
from jax.experimental.pallas import tpu as pltpu
from jax.sharding import PartitionSpec as P

masked_score = -1e30
LANES = 128
EXTRA = 2
PIECES = 3
STAGGER_NS = 5000
bf16 = jnp.bfloat16
f32 = jnp.float32
VMEM = pltpu.VMEM


def dot_nt(a, b):
    return lax.dot_general(a, b, (((1,), (1,)), ((), ())), preferred_element_type=f32)


def dot_nn(a, b):
    return lax.dot_general(a, b, (((1,), (0,)), ((), ())), preferred_element_type=f32)


def pieces(x):
    first = x.astype(bf16).astype(f32)
    rest = x - first
    second = rest.astype(bf16).astype(f32)
    third = (rest - second).astype(bf16).astype(f32)
    return first, second, third


def chunk_rows(d, h, rows, heads):
    at = d * (rows * heads + EXTRA) + h * rows
    return slice(at, at + (rows if h < heads else EXTRA))


def fold(x, rows):
    half, shift = rows // 2, LANES // 2
    while half >= EXTRA:
        x = x + pltpu.roll(pltpu.roll(x, rows - half, 0), shift, 1)
        half, shift = half // 2, shift // 2
    return x[:EXTRA, :]


def unfold(x, rows):
    step = LANES * EXTRA // rows
    parts = [x] + [pltpu.roll(x, LANES - i * step, 1) for i in range(1, rows // EXTRA)]
    return jnp.concatenate(parts, axis=0)


def pack_kernel(seq, tokens, q_hbm, owner_hbm, slot_hbm, len_hbm, out_ref, *scratch):
    q_ref, owner_ref, slot_ref, len_ref, sems, q_rows, table = scratch
    pairs = (len_hbm, len_ref), (owner_hbm, owner_ref), (slot_hbm, slot_ref), (q_hbm, q_ref)
    loads = [pltpu.make_async_copy(a, b, sems.at[i]) for i, (a, b) in enumerate(pairs)]
    for load in loads:
        load.start()
    rows, heads, width = q_ref.shape
    for load in loads[:3]:
        load.wait()
    pages = owner_ref.shape[1]
    place = lax.broadcasted_iota(jnp.int32, (1, pages), 1) * tokens
    owner_id = lax.broadcasted_iota(jnp.int32, (seq, pages), 0)
    slot_id = lax.broadcasted_iota(jnp.int32, (LANES, pages), 0)
    half = LANES // 2
    codes = None
    for r in range(rows):
        live = jnp.clip(len_ref[r] - place, 0, tokens).astype(f32)
        here = owner_ref[r : r + 1, :] == owner_id
        slot = slot_ref[r : r + 1, :]
        number = jnp.where(here, r + 1.0, 0.0).astype(bf16)
        count = jnp.where(here, live, 0.0).astype(bf16)
        low = jnp.where(slot == slot_id, 1.0, 0.0).astype(bf16)
        high = jnp.where(slot + half == slot_id, 1.0, 0.0).astype(bf16)
        both = dot_nt(
            jnp.concatenate([number, count], axis=1), jnp.concatenate([low, high], axis=1)
        )
        codes = both if codes is None else codes + both
    table[...] = jnp.zeros_like(table)
    table[pl.ds(0, seq, stride=EXTRA), :] = codes
    for d in range(seq):
        code = table[d * EXTRA : (d + 1) * EXTRA, :].astype(bf16)
        out_ref[chunk_rows(d, heads, rows, heads), :] = code

    @pl.when(lax.axis_index("rep") == 0)
    def _():
        pl.delay(STAGGER_NS)

    loads[3].wait()
    q_rows[...] = q_ref[...].astype(f32).reshape(rows * heads, width)
    for h in range(heads):
        part = q_rows[pl.ds(h, rows, stride=heads), :]
        part = part.astype(bf16)
        for d in range(seq):
            out_ref[chunk_rows(d, h, rows, heads), :] = part


def side_by_side(ref, p, heads):
    first = ref[p * heads : (p + 1) * heads, :]
    second = ref[(p + 1) * heads : (p + 2) * heads, :]
    none = jnp.zeros_like(first)
    left = jnp.concatenate([first, none], axis=0)
    right = jnp.concatenate([none, second], axis=0)
    return jnp.concatenate([left, right], axis=1).astype(bf16)


def pages_kernel(pool, heads, rows, in_ref, k_ref, v_ref, out_ref, qs, sc, po):
    width = k_ref.shape[2]
    tokens = k_ref.shape[1]
    seq = in_ref.shape[0] // (rows * heads + EXTRA)
    reqs = seq * rows
    number = lax.broadcasted_iota(jnp.int32, (rows, LANES), 0).astype(f32) + 1.0
    live_of = []
    for d in range(seq):
        code = in_ref[chunk_rows(d, heads, rows, heads), :].astype(f32)
        code = jnp.broadcast_to(code[:1, :], (rows, LANES))
        live_of.append(jnp.where(code == number, pltpu.roll(code, LANES // 2, 1), 0.0))
    live_of = jnp.concatenate(live_of, axis=0)
    live_by_page = live_of.T[:pool, :]
    linked_t = live_by_page > 0.0
    live = jnp.max(live_by_page, axis=1, keepdims=True)
    picker = jnp.where(linked_t, 1.0, 0.0).astype(bf16)
    for h in range(0, heads, 2):
        asked = [
            jnp.concatenate(
                [in_ref[chunk_rows(d, h + i, rows, heads), :].astype(f32) for d in range(seq)], axis=0
            )
            for i in range(2)
        ]
        slot_q = dot_nn(picker, jnp.concatenate(asked, axis=1).astype(bf16))
        for i in range(2):
            qs[pl.ds(h + i, pool, stride=heads), :] = slot_q[:, i * width : (i + 1) * width]
    for p in range(0, pool, 2):
        both = jnp.concatenate([k_ref[p], k_ref[p + 1]], axis=1)
        sc[p * heads : (p + 2) * heads, :] = dot_nt(side_by_side(qs, p, heads), both)
    scale = 1.0 / math.sqrt(width)
    mask = lax.broadcasted_iota(jnp.int32, (pool, tokens), 1).astype(f32) < live
    page_max, page_sum = [], []
    for h in range(heads):
        of_head = pl.ds(h, pool, stride=heads)
        s = jnp.where(mask, sc[of_head, :] * scale, masked_score)
        m = jnp.max(s, axis=1, keepdims=True)
        w = jnp.where(mask, jnp.exp(s - m), 0.0)
        sc[of_head, :] = w
        page_max.append(m)
        page_sum.append(jnp.sum(w, axis=1, keepdims=True))
    for p in range(0, pool, 2):
        both = v_ref[p : p + 2].reshape(2 * tokens, width)
        po[p * heads : (p + 2) * heads, :] = dot_nn(side_by_side(sc, p, heads), both)
    tops, sums, scaled = [], [], []
    for h in range(heads):
        top = jnp.max(jnp.where(linked_t, page_max[h], masked_score), axis=0, keepdims=True)
        page_top = jnp.max(jnp.where(linked_t, top, masked_score), axis=1, keepdims=True)
        rescale = jnp.exp(jnp.minimum(page_max[h] - page_top, 0.0))
        tops.append(top)
        sums.append(
            jnp.sum(jnp.where(linked_t, page_sum[h] * rescale, 0.0), axis=0, keepdims=True)
        )
        scaled.append(po[pl.ds(h, pool, stride=heads), :] * rescale)
    top = jnp.concatenate(tops, axis=0)
    total = jnp.concatenate(sums, axis=0)
    inverse = jnp.where(total > 0.0, 1.0 / jnp.where(total > 0.0, total, 1.0), 0.0)
    high, low, _ = pieces(top)
    total = total * jnp.exp(jnp.where(total > 0.0, top - (high + low), 0.0))
    filler = jnp.zeros((LANES - 5 * heads, reqs), f32)
    stats = jnp.concatenate([high, low, *pieces(total)[:2], inverse, filler], axis=0).T
    sent = lax.broadcasted_iota(jnp.int32, (rows, LANES), 1) < 4 * heads
    for d in range(seq):
        piece = jnp.where(sent, stats[d * rows : (d + 1) * rows, :], 0.0)
        out_ref[chunk_rows(d, heads, rows, heads), :] = fold(piece, rows).astype(bf16)
    linked = jnp.where(live_of[:, :pool] > 0.0, 1.0, 0.0).astype(bf16)
    linked = jnp.concatenate([linked] * PIECES, axis=1)
    for h in range(0, heads, 2):
        stack = [jnp.concatenate(pieces(x)[:PIECES], axis=0) for x in scaled[h : h + 2]]
        both = dot_nn(linked, jnp.concatenate(stack, axis=1).astype(bf16))
        for i in range(2):
            joined = both[:, i * width : (i + 1) * width]
            joined = joined * stats[:, 4 * heads + h + i : 4 * heads + h + i + 1]
            for d in range(seq):
                piece = joined[d * rows : (d + 1) * rows, :].astype(bf16)
                out_ref[chunk_rows(d, h + i, rows, heads), :] = piece


def merge_kernel(heads, rows, in_ref, out_ref, scratch):
    seq = in_ref.shape[0] // (rows * heads + EXTRA)
    stats = [
        unfold(in_ref[chunk_rows(d, heads, rows, heads), :].astype(f32), rows) for d in range(seq)
    ]
    stats = jnp.concatenate(stats, axis=0)
    joined = stats + pltpu.roll(stats, LANES - heads, 1)
    top = joined.reshape(seq, rows, LANES)
    total = pltpu.roll(joined, LANES - 2 * heads, 1).reshape(seq, rows, LANES)
    share = jnp.exp(top - jnp.max(top, axis=0, keepdims=True)) * total
    share = share * (1.0 / jnp.sum(share, axis=0, keepdims=True))
    share = share.reshape(seq * rows, LANES)
    for h in range(heads):
        total = None
        for d in range(seq):
            x = in_ref[chunk_rows(d, h, rows, heads), :].astype(f32)
            x = x * share[d * rows : (d + 1) * rows, h : h + 1]
            total = x if total is None else total + x
        scratch[pl.ds(h, rows, stride=heads), :] = total
    out_ref[...] = scratch[...].astype(bf16)


def on_device(queries, page_owner, page_slot, lengths, keys, values):
    rows, heads, width = queries.shape
    pool, _, tokens, _ = keys.shape
    seq = lax.axis_size("seq")
    reqs = seq * rows
    chunk = rows * heads + EXTRA
    whole = pl.BlockSpec(memory_space=VMEM)
    hbm = pl.BlockSpec(memory_space=pltpu.HBM)
    small = (queries, page_owner, page_slot, lengths)
    packed = pl.pallas_call(
        lambda *refs: pack_kernel(seq, tokens, *refs),
        out_shape=jax.ShapeDtypeStruct((seq * chunk, width), bf16),
        in_specs=[hbm] * 4,
        out_specs=whole,
        scratch_shapes=[
            VMEM(queries.shape, bf16),
            VMEM(page_owner.shape, jnp.int32),
            VMEM(page_slot.shape, jnp.int32),
            pltpu.SMEM(lengths.shape, jnp.int32),
            pltpu.SemaphoreType.DMA((4,)),
            VMEM((rows * heads, width), f32),
            VMEM((seq * EXTRA, LANES), f32),
        ],
        cost_estimate=pl.CostEstimate(flops=1 << 33, bytes_accessed=1 << 19, transcendentals=0),
        compiler_params=pltpu.CompilerParams(vmem_limit_bytes=4 << 20),
        name="pack",
    )(*[pltpu.with_memory_space_constraint(a, pltpu.HBM) for a in small])

    def exchange(x):
        x = x.reshape(seq, chunk // EXTRA, EXTRA, width)
        return lax.all_to_all(x, "seq", 0, 0, tiled=True).reshape(seq * chunk, width)

    got = exchange(packed)
    partial = pl.pallas_call(
        lambda *refs: pages_kernel(pool, heads, rows, *refs),
        out_shape=jax.ShapeDtypeStruct((seq * chunk, width), bf16),
        in_specs=[whole, whole, whole],
        out_specs=whole,
        scratch_shapes=[VMEM((pool * heads, width), f32)] * 3,
        compiler_params=pltpu.CompilerParams(vmem_limit_bytes=12 << 20),
        name="pages",
    )(got, keys.reshape(pool, tokens, width), values.reshape(pool, tokens, width))
    back = exchange(partial)
    out = pl.pallas_call(
        lambda *refs: merge_kernel(heads, rows, *refs),
        out_shape=jax.ShapeDtypeStruct((rows * heads, width), bf16),
        in_specs=[whole],
        out_specs=whole,
        scratch_shapes=[VMEM((rows * heads, width), f32)],
        compiler_params=pltpu.CompilerParams(vmem_limit_bytes=4 << 20),
        name="merge",
    )(back)
    return out.reshape(rows, heads, width)


def solution(mesh):
    placed = (
        P(("groups", "seq", "rep"), "head", None),
        P(("groups", "seq", "rep"), None),
        P(("groups", "seq", "rep"), None),
        P(("groups", "seq", "rep")),
        P(("groups", "seq", "rep"), "head", None, None),
        P(("groups", "seq", "rep"), "head", None, None),
    )
    return jax.shard_map(
        on_device,
        mesh=mesh,
        in_specs=placed,
        out_specs=P(("groups", "seq", "rep"), "head", None),
        check_vma=False,
    )
```

```python
import math

import jax
import jax.numpy as jnp
from jax import lax
from jax.experimental import pallas as pl
from jax.experimental.pallas import tpu as pltpu
from jax.sharding import PartitionSpec as P

masked_score = -1e30
LANES = 128
EXTRA = 2
PIECES = 2
STAGGER_NS = 5000
bf16 = jnp.bfloat16
f32 = jnp.float32
VMEM = pltpu.VMEM


def dot_nt(a, b):
    return lax.dot_general(a, b, (((1,), (1,)), ((), ())), preferred_element_type=f32)


def dot_nn(a, b):
    return lax.dot_general(a, b, (((1,), (0,)), ((), ())), preferred_element_type=f32)


def pieces(x):
    first = x.astype(bf16).astype(f32)
    rest = x - first
    second = rest.astype(bf16).astype(f32)
    third = (rest - second).astype(bf16).astype(f32)
    return first, second, third


def chunk_rows(d, h, rows, heads):
    at = d * (rows * heads + EXTRA) + h * rows
    return slice(at, at + (rows if h < heads else EXTRA))


def fold(x, rows):
    half, shift = rows // 2, LANES // 2
    while half >= EXTRA:
        x = x + pltpu.roll(pltpu.roll(x, rows - half, 0), shift, 1)
        half, shift = half // 2, shift // 2
    return x[:EXTRA, :]


def unfold(x, rows):
    step = LANES * EXTRA // rows
    parts = [x] + [pltpu.roll(x, LANES - i * step, 1) for i in range(1, rows // EXTRA)]
    return jnp.concatenate(parts, axis=0)


def pack_kernel(seq, tokens, q_hbm, owner_hbm, slot_hbm, len_hbm, out_ref, *scratch):
    q_ref, owner_ref, slot_ref, len_ref, sems, q_rows, table = scratch
    pairs = (len_hbm, len_ref), (owner_hbm, owner_ref), (slot_hbm, slot_ref), (q_hbm, q_ref)
    loads = [pltpu.make_async_copy(a, b, sems.at[i]) for i, (a, b) in enumerate(pairs)]
    for load in loads:
        load.start()
    rows, heads, width = q_ref.shape
    for load in loads[:3]:
        load.wait()
    pages = owner_ref.shape[1]
    place = lax.broadcasted_iota(jnp.int32, (1, pages), 1) * tokens
    owner_id = lax.broadcasted_iota(jnp.int32, (seq, pages), 0)
    slot_id = lax.broadcasted_iota(jnp.int32, (LANES, pages), 0)
    half = LANES // 2
    codes = None
    for r in range(rows):
        live = jnp.clip(len_ref[r] - place, 0, tokens).astype(f32)
        here = owner_ref[r : r + 1, :] == owner_id
        slot = slot_ref[r : r + 1, :]
        number = jnp.where(here, r + 1.0, 0.0).astype(bf16)
        count = jnp.where(here, live, 0.0).astype(bf16)
        low = jnp.where(slot == slot_id, 1.0, 0.0).astype(bf16)
        high = jnp.where(slot + half == slot_id, 1.0, 0.0).astype(bf16)
        both = dot_nt(
            jnp.concatenate([number, count], axis=1), jnp.concatenate([low, high], axis=1)
        )
        codes = both if codes is None else codes + both
    table[...] = jnp.zeros_like(table)
    table[pl.ds(0, seq, stride=EXTRA), :] = codes
    for d in range(seq):
        code = table[d * EXTRA : (d + 1) * EXTRA, :].astype(bf16)
        out_ref[chunk_rows(d, heads, rows, heads), :] = code

    @pl.when(lax.axis_index("rep") == 0)
    def _():
        pl.delay(STAGGER_NS)

    loads[3].wait()
    q_rows[...] = q_ref[...].astype(f32).reshape(rows * heads, width)
    for h in range(heads):
        part = q_rows[pl.ds(h, rows, stride=heads), :]
        part = part.astype(bf16)
        for d in range(seq):
            out_ref[chunk_rows(d, h, rows, heads), :] = part


def side_by_side(ref, p, heads):
    first = ref[p * heads : (p + 1) * heads, :]
    second = ref[(p + 1) * heads : (p + 2) * heads, :]
    none = jnp.zeros_like(first)
    left = jnp.concatenate([first, none], axis=0)
    right = jnp.concatenate([none, second], axis=0)
    return jnp.concatenate([left, right], axis=1).astype(bf16)


def pages_kernel(pool, heads, rows, in_ref, k_ref, v_ref, out_ref, qs, sc, po):
    width = k_ref.shape[2]
    tokens = k_ref.shape[1]
    seq = in_ref.shape[0] // (rows * heads + EXTRA)
    reqs = seq * rows
    number = lax.broadcasted_iota(jnp.int32, (rows, LANES), 0).astype(f32) + 1.0
    live_of = []
    for d in range(seq):
        code = in_ref[chunk_rows(d, heads, rows, heads), :].astype(f32)
        code = jnp.broadcast_to(code[:1, :], (rows, LANES))
        live_of.append(jnp.where(code == number, pltpu.roll(code, LANES // 2, 1), 0.0))
    live_of = jnp.concatenate(live_of, axis=0)
    live_by_page = live_of.T[:pool, :]
    linked_t = live_by_page > 0.0
    live = jnp.max(live_by_page, axis=1, keepdims=True)
    picker = jnp.where(linked_t, 1.0, 0.0).astype(bf16)
    for h in range(0, heads, 2):
        asked = [
            jnp.concatenate(
                [in_ref[chunk_rows(d, h + i, rows, heads), :].astype(f32) for d in range(seq)], axis=0
            )
            for i in range(2)
        ]
        slot_q = dot_nn(picker, jnp.concatenate(asked, axis=1).astype(bf16))
        for i in range(2):
            qs[pl.ds(h + i, pool, stride=heads), :] = slot_q[:, i * width : (i + 1) * width]
    for p in range(0, pool, 2):
        both = jnp.concatenate([k_ref[p], k_ref[p + 1]], axis=1)
        sc[p * heads : (p + 2) * heads, :] = dot_nt(side_by_side(qs, p, heads), both)
    scale = 1.0 / math.sqrt(width)
    mask = lax.broadcasted_iota(jnp.int32, (pool, tokens), 1).astype(f32) < live
    page_max, page_sum = [], []
    for h in range(heads):
        of_head = pl.ds(h, pool, stride=heads)
        s = jnp.where(mask, sc[of_head, :] * scale, masked_score)
        m = jnp.max(s, axis=1, keepdims=True)
        w = jnp.where(mask, jnp.exp(s - m), 0.0)
        sc[of_head, :] = w
        page_max.append(m)
        page_sum.append(jnp.sum(w, axis=1, keepdims=True))
    for p in range(0, pool, 2):
        both = v_ref[p : p + 2].reshape(2 * tokens, width)
        po[p * heads : (p + 2) * heads, :] = dot_nn(side_by_side(sc, p, heads), both)
    tops, sums, scaled = [], [], []
    for h in range(heads):
        top = jnp.max(jnp.where(linked_t, page_max[h], masked_score), axis=0, keepdims=True)
        page_top = jnp.max(jnp.where(linked_t, top, masked_score), axis=1, keepdims=True)
        rescale = jnp.exp(jnp.minimum(page_max[h] - page_top, 0.0))
        tops.append(top)
        sums.append(
            jnp.sum(jnp.where(linked_t, page_sum[h] * rescale, 0.0), axis=0, keepdims=True)
        )
        scaled.append(po[pl.ds(h, pool, stride=heads), :] * rescale)
    top = jnp.concatenate(tops, axis=0)
    total = jnp.concatenate(sums, axis=0)
    inverse = jnp.where(total > 0.0, 1.0 / jnp.where(total > 0.0, total, 1.0), 0.0)
    high, low, _ = pieces(top)
    total = total * jnp.exp(jnp.where(total > 0.0, top - (high + low), 0.0))
    filler = jnp.zeros((LANES - 5 * heads, reqs), f32)
    stats = jnp.concatenate([high, low, *pieces(total)[:2], inverse, filler], axis=0).T
    sent = lax.broadcasted_iota(jnp.int32, (rows, LANES), 1) < 4 * heads
    for d in range(seq):
        piece = jnp.where(sent, stats[d * rows : (d + 1) * rows, :], 0.0)
        out_ref[chunk_rows(d, heads, rows, heads), :] = fold(piece, rows).astype(bf16)
    linked = jnp.where(live_of[:, :pool] > 0.0, 1.0, 0.0).astype(bf16)
    linked = jnp.concatenate([linked] * PIECES, axis=1)
    for h in range(0, heads, 2):
        stack = [jnp.concatenate(pieces(x)[:PIECES], axis=0) for x in scaled[h : h + 2]]
        both = dot_nn(linked, jnp.concatenate(stack, axis=1).astype(bf16))
        for i in range(2):
            joined = both[:, i * width : (i + 1) * width]
            joined = joined * stats[:, 4 * heads + h + i : 4 * heads + h + i + 1]
            for d in range(seq):
                piece = joined[d * rows : (d + 1) * rows, :].astype(bf16)
                out_ref[chunk_rows(d, h + i, rows, heads), :] = piece


def merge_kernel(heads, rows, in_ref, out_ref, scratch):
    seq = in_ref.shape[0] // (rows * heads + EXTRA)
    stats = [
        unfold(in_ref[chunk_rows(d, heads, rows, heads), :].astype(f32), rows) for d in range(seq)
    ]
    stats = jnp.concatenate(stats, axis=0)
    joined = stats + pltpu.roll(stats, LANES - heads, 1)
    top = joined.reshape(seq, rows, LANES)
    total = pltpu.roll(joined, LANES - 2 * heads, 1).reshape(seq, rows, LANES)
    share = jnp.exp(top - jnp.max(top, axis=0, keepdims=True)) * total
    share = share * (1.0 / jnp.sum(share, axis=0, keepdims=True))
    share = share.reshape(seq * rows, LANES)
    for h in range(heads):
        total = None
        for d in range(seq):
            x = in_ref[chunk_rows(d, h, rows, heads), :].astype(f32)
            x = x * share[d * rows : (d + 1) * rows, h : h + 1]
            total = x if total is None else total + x
        scratch[pl.ds(h, rows, stride=heads), :] = total
    out_ref[...] = scratch[...].astype(bf16)


def on_device(queries, page_owner, page_slot, lengths, keys, values):
    rows, heads, width = queries.shape
    pool, _, tokens, _ = keys.shape
    seq = lax.axis_size("seq")
    reqs = seq * rows
    chunk = rows * heads + EXTRA
    whole = pl.BlockSpec(memory_space=VMEM)
    hbm = pl.BlockSpec(memory_space=pltpu.HBM)
    small = (queries, page_owner, page_slot, lengths)
    packed = pl.pallas_call(
        lambda *refs: pack_kernel(seq, tokens, *refs),
        out_shape=jax.ShapeDtypeStruct((seq * chunk, width), bf16),
        in_specs=[hbm] * 4,
        out_specs=whole,
        scratch_shapes=[
            VMEM(queries.shape, bf16),
            VMEM(page_owner.shape, jnp.int32),
            VMEM(page_slot.shape, jnp.int32),
            pltpu.SMEM(lengths.shape, jnp.int32),
            pltpu.SemaphoreType.DMA((4,)),
            VMEM((rows * heads, width), f32),
            VMEM((seq * EXTRA, LANES), f32),
        ],
        cost_estimate=pl.CostEstimate(flops=1 << 33, bytes_accessed=1 << 19, transcendentals=0),
        compiler_params=pltpu.CompilerParams(vmem_limit_bytes=4 << 20),
        name="pack",
    )(*[pltpu.with_memory_space_constraint(a, pltpu.HBM) for a in small])

    def exchange(x):
        x = x.reshape(seq, chunk // EXTRA, EXTRA, width)
        return lax.all_to_all(x, "seq", 0, 0, tiled=True).reshape(seq * chunk, width)

    got = exchange(packed)
    partial = pl.pallas_call(
        lambda *refs: pages_kernel(pool, heads, rows, *refs),
        out_shape=jax.ShapeDtypeStruct((seq * chunk, width), bf16),
        in_specs=[whole, whole, whole],
        out_specs=whole,
        scratch_shapes=[VMEM((pool * heads, width), f32)] * 3,
        compiler_params=pltpu.CompilerParams(
            vmem_limit_bytes=12 << 20
        ),
        name="pages",
    )(got, keys.reshape(pool, tokens, width), values.reshape(pool, tokens, width))
    back = exchange(partial)
    out = pl.pallas_call(
        lambda *refs: merge_kernel(heads, rows, *refs),
        out_shape=jax.ShapeDtypeStruct((rows * heads, width), bf16),
        in_specs=[whole],
        out_specs=whole,
        scratch_shapes=[VMEM((rows * heads, width), f32)],
        compiler_params=pltpu.CompilerParams(vmem_limit_bytes=4 << 20),
        name="merge",
    )(back)
    return out.reshape(rows, heads, width)


def solution(mesh):
    placed = (
        P(("groups", "seq", "rep"), "head", None),
        P(("groups", "seq", "rep"), None),
        P(("groups", "seq", "rep"), None),
        P(("groups", "seq", "rep")),
        P(("groups", "seq", "rep"), "head", None, None),
        P(("groups", "seq", "rep"), "head", None, None),
    )
    return jax.shard_map(
        on_device,
        mesh=mesh,
        in_specs=placed,
        out_specs=P(("groups", "seq", "rep"), "head", None),
        check_vma=False,
    )
```
